32 devices in a mesh: gz: 32 (over z, y, x, core).
Axes of the slice: x: 2, y: 2, z: 4, core: 2. Of those that a mesh axis runs over, the one named last changes fastest.
Arguments:
- density: float32 [2, 32, 256, 256], P(None, 'gz'), may hold values from 0.02 to 0.8
- kernel_hat: float32 [64, 512, 512], P(None, 'gz'), may hold values from 0.37 to 7, as said below
Outputs:
- potential: float32 [2, 32, 256, 256], P(None, 'gz')
- energies: float32 [2], replicated
The draws below stay inside these ranges and needn't reach their ends.
Inputs may be any that keep to these rules, and one draw needn't show every extreme that they name: kernel_hat at (a, b, c) equals kernel_hat at ((-a) mod 64, (-b) mod 512, (-c) mod 512).
All inputs are finite; a program needn't handle non-finite values.
Results may differ from the reference program's by a relative error of at most 0.00015.
Values sent between devices are 32-bit elements; how exact they have to be, the bound alone decides.
A program may use at most 64 MiB of HBM per device.

```python
import math
import jax
import jax.numpy as jnp
from jax import lax

NX = 256
NY = 256
NZ = 32
MX = 512
MY = 512
MZ = 64


SCREEN = 0.01


STRENGTH = 0.02


CONTACT = 1.5


def draw_density(key, part):
    height = jnp.arange(NZ, dtype=jnp.float32)[None, :, None, None] / max(NZ - 1, 1)
    uniform_draw = jax.random.uniform(key, (2, NZ, NY, NX), jnp.float32)
    ramp_values = 0.1 * jnp.exp(math.log(4.5) * height)
    return ramp_values * 0.3 * jnp.exp(math.log(5.0) * uniform_draw)


def symbol(length_cells):
    indices = jnp.arange(length_cells, dtype=jnp.int32)
    folded = jnp.minimum(indices, length_cells - indices).astype(jnp.float32)
    return (2.0 * jnp.sin(math.pi * folded / length_cells)) ** 2


def draw_kernel_hat(key, part):
    laplace = symbol(MZ)[:, None, None] + symbol(MY)[None, :, None] + symbol(MX)[None, None, :]
    uniform_draw = jax.random.uniform(key, (MZ, MY, MX), jnp.float32)
    roughness = jnp.exp(math.log(0.5) + math.log(4.0) * uniform_draw)
    mirrored = roughness
    for direction in range(3):
        mirrored = jnp.roll(jnp.flip(mirrored, direction), 1, direction)
    return (STRENGTH / (laplace + SCREEN) + CONTACT) * (0.5 * (roughness + mirrored))


def setup_inputs(seed: int = 0) -> dict:
    key_list = jax.random.split(jax.random.key(seed), 3)
    density = draw_density(jax.random.fold_in(key_list[2], 71), 0)
    kernel_hat = draw_kernel_hat(jax.random.fold_in(key_list[2], 71), 0)
    return {"density": density, "kernel_hat": kernel_hat}


HGRID = 0.35
STENCIL = (0.8, -0.2, 4.0 / 105.0, -1.0 / 280.0)
KAPPA = 0.804
MU_X = 0.2195149727645171
BETA_C = 0.06672455060314922
GAMMA_C = 0.031090690869654894
FZ_CURV = 1.709921
PARAMS_UNPOL = (0.031091, 0.2137, 7.5957, 3.5876, 1.6382, 0.49294)
PARAMS_POL = (0.015545, 0.20548, 14.1189, 6.1977, 3.3662, 0.62517)
PARAMS_STIFF = (0.016887, 0.11125, 10.357, 3.6231, 0.88026, 0.49671)

def inner_slope(extended, direction):
    stencil_reach = len(STENCIL)
    length_out = extended.shape[direction] - 2 * stencil_reach
    result = 0.0
    for offset, weight in enumerate(STENCIL):
        upper_part = lax.slice_in_dim(extended, stencil_reach + offset + 1, stencil_reach + offset + 1 + length_out, axis=direction)
        lower_part = lax.slice_in_dim(extended, stencil_reach - offset - 1, stencil_reach - offset - 1 + length_out, axis=direction)
        result = result + weight * (upper_part - lower_part)
    return result / HGRID

def plane_slope(field, direction):
    stencil_reach = len(STENCIL)
    widths = [(0, 0)] * field.ndim
    widths[direction] = (stencil_reach, stencil_reach)
    return inner_slope(jnp.pad(field, widths), direction)

def pw_piece(radius, params):
    half_root = jnp.sqrt(radius)
    series = params[2] * half_root + params[3] * radius + params[4] * radius * half_root + params[5] * radius * radius
    return -2.0 * params[0] * (1.0 + params[1] * radius) * jnp.log1p(1.0 / (2.0 * params[0] * series))

def exchange_part(doubled, sigma_four):
    cube_root = jnp.cbrt(doubled)
    uniform_part = -0.75 * (3.0 / math.pi) ** (1.0 / 3.0) * cube_root
    reduced = sigma_four / (4.0 * (3.0 * math.pi ** 2) ** (2.0 / 3.0) * doubled ** 2 * cube_root ** 2)
    enhance = 1.0 + KAPPA - KAPPA / (1.0 + MU_X * reduced / KAPPA)
    return doubled * uniform_part * enhance

def energy_density(dens_up, dens_down, sigma_uu, sigma_ud, sigma_dd):
    exchange_term = 0.5 * exchange_part(2.0 * dens_up, 4.0 * sigma_uu) + 0.5 * exchange_part(2.0 * dens_down, 4.0 * sigma_dd)
    density_sum = dens_up + dens_down
    polarization = (dens_up - dens_down) / density_sum
    radius = jnp.cbrt(3.0 / (4.0 * math.pi * density_sum))
    plus_side = 1.0 + polarization
    minus_side = 1.0 - polarization
    plus_cube = jnp.cbrt(plus_side)
    minus_cube = jnp.cbrt(minus_side)
    spin_weight = (plus_side * plus_cube + minus_side * minus_cube - 2.0) / (2.0 ** (4.0 / 3.0) - 2.0)
    unpolar = pw_piece(radius, PARAMS_UNPOL)
    polarized = pw_piece(radius, PARAMS_POL)
    stiffness = pw_piece(radius, PARAMS_STIFF)
    polar_four = polarization ** 4
    local_corr = unpolar - stiffness * spin_weight * (1.0 - polar_four) / FZ_CURV + (polarized - unpolar) * spin_weight * polar_four
    phi_factor = 0.5 * (plus_cube ** 2 + minus_cube ** 2)
    phi_cubed = phi_factor ** 3
    screening_sq = 4.0 * jnp.cbrt(3.0 * math.pi ** 2 * density_sum) / math.pi
    sigma_total = sigma_uu + 2.0 * sigma_ud + sigma_dd
    scaled_sq = sigma_total / (4.0 * phi_factor ** 2 * screening_sq * density_sum ** 2)
    weight_a = BETA_C / GAMMA_C / jnp.expm1(-local_corr / (GAMMA_C * phi_cubed))
    gradient_term = GAMMA_C * phi_cubed * jnp.log1p(BETA_C / GAMMA_C * scaled_sq * (1.0 + weight_a * scaled_sq) / (1.0 + weight_a * scaled_sq + weight_a ** 2 * scaled_sq ** 2))
    return exchange_term + density_sum * (local_corr + gradient_term)

def flux_pair(deriv_uu, deriv_ud, deriv_dd, gradient):
    return jnp.stack([2.0 * deriv_uu * gradient[0] + deriv_ud * gradient[1], 2.0 * deriv_dd * gradient[1] + deriv_ud * gradient[0]])

def xc_fields(dens, grad_z, grad_y, grad_x):
    sigma_uu = grad_z[0] * grad_z[0] + grad_y[0] * grad_y[0] + grad_x[0] * grad_x[0]
    sigma_ud = grad_z[0] * grad_z[1] + grad_y[0] * grad_y[1] + grad_x[0] * grad_x[1]
    sigma_dd = grad_z[1] * grad_z[1] + grad_y[1] * grad_y[1] + grad_x[1] * grad_x[1]
    energy, pullback = jax.vjp(energy_density, dens[0], dens[1], sigma_uu, sigma_ud, sigma_dd)
    d_up, d_down, d_uu, d_ud, d_dd = pullback(jnp.ones_like(energy))
    return (energy, jnp.stack([d_up, d_down]), flux_pair(d_uu, d_ud, d_dd, grad_z), flux_pair(d_uu, d_ud, d_dd, grad_y), flux_pair(d_uu, d_ud, d_dd, grad_x))

def plane_terms(slices):
    density_plane, grad_z, grad_y, grad_x = slices
    return xc_fields(density_plane, grad_z, grad_y, grad_x)

def reference(density, kernel_hat):
    grad_z = plane_slope(density, 1)
    grad_y = plane_slope(density, 2)
    grad_x = plane_slope(density, 3)
    moved = tuple((jnp.moveaxis(array_item, 1, 0) for array_item in (density, grad_z, grad_y, grad_x)))
    energy, d_dens, flux_z, flux_y, flux_x = lax.map(plane_terms, moved)
    d_dens = jnp.moveaxis(d_dens, 0, 1)
    flux_z = jnp.moveaxis(flux_z, 0, 1)
    flux_y = jnp.moveaxis(flux_y, 0, 1)
    flux_x = jnp.moveaxis(flux_x, 0, 1)
    v_xc = d_dens - (plane_slope(flux_z, 1) + plane_slope(flux_y, 2) + plane_slope(flux_x, 3))
    density_sum = density[0] + density[1]
    padded = jnp.pad(density_sum, ((0, NZ), (0, NY), (0, NX)))
    spectrum = jnp.fft.rfftn(padded)
    filtered = jnp.fft.irfftn(spectrum * kernel_hat[:, :, :NX + 1], s=padded.shape)
    hartree = filtered[:NZ, :NY, :NX]
    potential = v_xc + hartree[None]
    energies = jnp.stack([jnp.mean(energy), 0.5 * jnp.mean(density_sum * hartree)])
    return (potential, energies)
```

```python
import functools
import math

import jax
import jax.numpy as jnp
import numpy as np
from jax import lax
from jax.experimental import pallas as pl
from jax.experimental.pallas import tpu as pltpu
from jax.sharding import PartitionSpec as P

HGRID = 0.35
STENCIL = (0.8, -0.2, 4.0 / 105.0, -1.0 / 280.0)
KAPPA = 0.804
MU_X = 0.2195149727645171
BETA_C = 0.06672455060314922
GAMMA_C = 0.031090690869654894
FZ_CURV = 1.709921
PARAMS_UNPOL = (0.031091, 0.2137, 7.5957, 3.5876, 1.6382, 0.49294)
PARAMS_POL = (0.015545, 0.20548, 14.1189, 6.1977, 3.3662, 0.62517)
PARAMS_STIFF = (0.016887, 0.11125, 10.357, 3.6231, 0.88026, 0.49671)


def shifted(value, axis, steps):
    count = lax.axis_size(axis)
    leading, last = (max(0, -steps), min(count, count - steps))
    return lax.ppermute(value, axis, [(source, source + steps) for source in range(leading, last)])


def inner_slope(extended, direction):
    stencil_reach = len(STENCIL)
    length_out = extended.shape[direction] - 2 * stencil_reach
    result = 0.0
    for offset, weight in enumerate(STENCIL):
        upper_part = lax.slice_in_dim(
            extended,
            stencil_reach + offset + 1,
            stencil_reach + offset + 1 + length_out,
            axis=direction,
        )
        lower_part = lax.slice_in_dim(
            extended,
            stencil_reach - offset - 1,
            stencil_reach - offset - 1 + length_out,
            axis=direction,
        )
        result = result + weight * (upper_part - lower_part)
    return result / HGRID


def plane_slope(field, direction):
    stencil_reach = len(STENCIL)
    widths = [(0, 0)] * field.ndim
    widths[direction] = (stencil_reach, stencil_reach)
    return inner_slope(jnp.pad(field, widths), direction)


def pw_piece(radius, params):
    half_root = jnp.sqrt(radius)
    series = (
        params[2] * half_root
        + params[3] * radius
        + params[4] * radius * half_root
        + params[5] * radius * radius
    )
    return (
        -2.0 * params[0] * (1.0 + params[1] * radius) * jnp.log1p(1.0 / (2.0 * params[0] * series))
    )


def exchange_part(doubled, sigma_four):
    cube_root = jnp.cbrt(doubled)
    uniform_part = -0.75 * (3.0 / math.pi) ** (1.0 / 3.0) * cube_root
    reduced = sigma_four / (4.0 * (3.0 * math.pi**2) ** (2.0 / 3.0) * doubled**2 * cube_root**2)
    enhance = 1.0 + KAPPA - KAPPA / (1.0 + MU_X * reduced / KAPPA)
    return doubled * uniform_part * enhance


def energy_density(dens_up, dens_down, sigma_uu, sigma_ud, sigma_dd):
    exchange_term = 0.5 * exchange_part(2.0 * dens_up, 4.0 * sigma_uu) + 0.5 * exchange_part(
        2.0 * dens_down, 4.0 * sigma_dd
    )
    density_sum = dens_up + dens_down
    polarization = (dens_up - dens_down) / density_sum
    radius = jnp.cbrt(3.0 / (4.0 * math.pi * density_sum))
    plus_side = 1.0 + polarization
    minus_side = 1.0 - polarization
    plus_cube = jnp.cbrt(plus_side)
    minus_cube = jnp.cbrt(minus_side)
    spin_weight = (plus_side * plus_cube + minus_side * minus_cube - 2.0) / (
        2.0 ** (4.0 / 3.0) - 2.0
    )
    unpolar = pw_piece(radius, PARAMS_UNPOL)
    polarized = pw_piece(radius, PARAMS_POL)
    stiffness = pw_piece(radius, PARAMS_STIFF)
    polar_four = polarization**4
    local_corr = (
        unpolar
        - stiffness * spin_weight * (1.0 - polar_four) / FZ_CURV
        + (polarized - unpolar) * spin_weight * polar_four
    )
    phi_factor = 0.5 * (plus_cube**2 + minus_cube**2)
    phi_cubed = phi_factor**3
    screening_sq = 4.0 * jnp.cbrt(3.0 * math.pi**2 * density_sum) / math.pi
    sigma_total = sigma_uu + 2.0 * sigma_ud + sigma_dd
    scaled_sq = sigma_total / (4.0 * phi_factor**2 * screening_sq * density_sum**2)
    weight_a = BETA_C / GAMMA_C / jnp.expm1(-local_corr / (GAMMA_C * phi_cubed))
    gradient_term = (
        GAMMA_C
        * phi_cubed
        * jnp.log1p(
            BETA_C
            / GAMMA_C
            * scaled_sq
            * (1.0 + weight_a * scaled_sq)
            / (1.0 + weight_a * scaled_sq + weight_a**2 * scaled_sq**2)
        )
    )
    return exchange_term + density_sum * (local_corr + gradient_term)


def flux_pair(deriv_uu, deriv_ud, deriv_dd, gradient):
    return jnp.stack(
        [
            2.0 * deriv_uu * gradient[0] + deriv_ud * gradient[1],
            2.0 * deriv_dd * gradient[1] + deriv_ud * gradient[0],
        ]
    )


def xc_fields(dens, grad_z, grad_y, grad_x):
    sigma_uu = grad_z[0] * grad_z[0] + grad_y[0] * grad_y[0] + grad_x[0] * grad_x[0]
    sigma_ud = grad_z[0] * grad_z[1] + grad_y[0] * grad_y[1] + grad_x[0] * grad_x[1]
    sigma_dd = grad_z[1] * grad_z[1] + grad_y[1] * grad_y[1] + grad_x[1] * grad_x[1]
    energy, pullback = jax.vjp(energy_density, dens[0], dens[1], sigma_uu, sigma_ud, sigma_dd)
    d_up, d_down, d_uu, d_ud, d_dd = pullback(jnp.ones_like(energy))
    return (
        energy,
        jnp.stack([d_up, d_down]),
        flux_pair(d_uu, d_ud, d_dd, grad_z),
        flux_pair(d_uu, d_ud, d_dd, grad_y),
        flux_pair(d_uu, d_ud, d_dd, grad_x),
    )


MESH = pl.DeviceIdType.MESH
LANES = 128
SUBLANES = 8
VMEM_SPEC = pl.BlockSpec(memory_space=pltpu.VMEM)
VMEM_BYTES = 60 * 1024 * 1024


def extend_rows(field, depth):
    rows = field.shape[2]
    below_parts = []
    above_parts = []
    for distance in range(1, -(-depth // rows) + 1):
        needed = min(rows, depth - (distance - 1) * rows)
        below_parts.insert(0, shifted(field[:, :, rows - needed :], "gz", distance))
        above_parts.append(shifted(field[:, :, :needed], "gz", -distance))
    return jnp.concatenate(below_parts + [field] + above_parts, axis=2)


def split(value):
    high = value.astype(jnp.bfloat16)
    low = (value - high.astype(jnp.float32)).astype(jnp.bfloat16)
    return high, low


def np_split(table):
    table = np.asarray(table, np.float32)
    high = table.astype(jnp.bfloat16)
    low = (table - high.astype(np.float32)).astype(jnp.bfloat16)
    return high, low


def angles(spatial, spectral):
    index = np.outer(np.arange(spatial), np.arange(spectral)) % spectral
    return index * (2.0 * np.pi / spectral)


def y_tables(width_y, devices, scale):
    angle = angles(width_y, 2 * width_y)
    both = np.stack([np.cos(angle), -np.sin(angle)])
    both = both.reshape(2, width_y, devices, -1).transpose(2, 0, 3, 1)
    forward = both.reshape(4 * width_y, width_y)
    return np_split(forward), np_split(forward.T * scale)


def x_table(width_x):
    angle = angles(width_x, 2 * width_x)[:, :width_x]
    sine = np.sin(angle)
    sine[:, 0] = (-1.0) ** np.arange(width_x)
    return np_split(np.concatenate([np.cos(angle), sine], axis=1))


def z_tables(depth_z):
    angle = angles(depth_z, 2 * depth_z)
    cos, sin = np.cos(angle).T, np.sin(angle).T
    forward = np.block([[cos, sin], [-sin, cos]])
    out = []
    for table in (forward, forward.T):
        high, low = np_split(table)
        out.append(np.concatenate([high, high, low], axis=1))
    return out


def dot(left, right):
    return jnp.dot(left, right, preferred_element_type=jnp.float32)


def stacked(value):
    high, low = split(value)
    return jnp.concatenate([high, low, high], axis=0)


def greet(devices):
    me = lax.axis_index("gz")
    barrier = pltpu.get_barrier_semaphore()

    def signal(step, carry):
        pl.semaphore_signal(
            barrier,
            inc=1,
            device_id=(lax.rem(me + step, devices),),
            device_id_type=MESH,
        )
        return carry

    lax.fori_loop(1, devices, signal, 0)
    return lambda: pl.semaphore_wait(barrier, devices - 1)


def remote(devices, pieces, sends, receives):
    me = lax.axis_index("gz")

    def each(step, source_of, slot_of, act):
        for piece, (source, target) in enumerate(pieces):
            act(
                pltpu.make_async_remote_copy(
                    src_ref=source(source_of),
                    dst_ref=target(slot_of),
                    send_sem=sends.at[piece, step],
                    recv_sem=receives.at[piece, step],
                    device_id=(source_of,),
                    device_id_type=MESH,
                )
            )

    def start(step, carry):
        each(step, lax.rem(me + step, devices), me, lambda copy: copy.start())
        return carry

    def finish(step, carry):
        peer = lax.rem(me + step, devices)
        origin = lax.rem(me - step + devices, devices)
        each(step, peer, me, lambda copy: copy.wait_send())
        each(step, peer, origin, lambda copy: copy.wait_recv())
        return carry

    lax.fori_loop(1, devices, start, 0)
    return lambda: lax.fori_loop(1, devices, finish, 0)


def forward_kernel(devices, dens, t_high, t_low, dens_out, spec_out, spec, sends, receives):
    me = lax.axis_index("gz")
    arrived = greet(devices)
    width_y = t_high.shape[1]
    total = (dens[0] + dens[1]).reshape(width_y, dens.shape[3])
    high, low = split(total)
    values = dot(t_high[...], high) + (dot(t_high[...], low) + dot(t_low[...], high))
    spec[...] = values.reshape(spec.shape)
    arrived()
    finish = remote(
        devices,
        [
            (lambda peer: dens.at[:, peer], lambda slot: dens_out.at[:, slot]),
            (lambda peer: spec.at[peer], lambda slot: spec_out.at[slot]),
        ],
        sends,
        receives,
    )
    dens_out[:, me] = dens[:, me]
    spec_out[me] = spec[me]
    finish()


def forward_exchange(devices, dens, tables):
    width_x = dens.shape[3]
    spec_shape = (devices, tables[0].shape[0] // devices, width_x)
    return pl.pallas_call(
        functools.partial(forward_kernel, devices),
        out_shape=(
            jax.ShapeDtypeStruct(dens.shape, jnp.float32),
            jax.ShapeDtypeStruct(spec_shape, jnp.float32),
        ),
        in_specs=[VMEM_SPEC] * 3,
        out_specs=(VMEM_SPEC, VMEM_SPEC),
        scratch_shapes=[
            pltpu.VMEM(spec_shape, jnp.float32),
            pltpu.SemaphoreType.DMA((2, devices)),
            pltpu.SemaphoreType.DMA((2, devices)),
        ],
        compiler_params=pltpu.CompilerParams(
            collective_id=0, has_side_effects=True, vmem_limit_bytes=VMEM_BYTES
        ),
        name="forward_exchange",
    )(dens, *tables)


def filter_kernel(spec, kernel_hat, edge, tx_high, tx_low, z_fore, z_back, out, energy, held, wide):
    depth, rows, width = spec.shape
    count = rows // 2
    for q in range(count):
        held[q, :depth] = spec[:, q, :]
        held[q, depth:] = spec[:, count + q, :]

    def times_x(value):
        high, low = split(value.reshape(count * 2 * depth, width))
        result = dot(high, tx_high[...]) + (dot(low, tx_high[...]) + dot(high, tx_low[...]))
        wide[...] = result.reshape(wide.shape)

    lane = lax.broadcasted_iota(jnp.int32, (1, width), 1)
    first = lane == 0
    weight = jnp.where(first, 1.0, 2.0)
    alternate = jnp.where(lane % 2 == 0, 1.0, -1.0)
    edge_lane = lax.broadcasted_iota(jnp.int32, (1, LANES), 1)
    times_x(held[...])
    last = jnp.zeros((2 * depth, LANES), jnp.float32)
    back = []
    for q in range(count):
        cos_part = wide[q, :, :width]
        sin_part = wide[q, :, width:]
        last = jnp.where(edge_lane == q, sin_part[:, :1], last)
        sin_part = jnp.where(first, 0.0, sin_part)
        value = jnp.concatenate(
            [cos_part[:depth] + sin_part[depth:], cos_part[depth:] - sin_part[:depth]], axis=0
        )
        value = dot(z_fore[...], stacked(value))
        factor = kernel_hat[:, q, :] * weight
        value = value * jnp.concatenate([factor, factor], axis=0)
        wide[q, :, :width] = dot(z_back[...], stacked(value))
    last = dot(z_fore[...], stacked(last))
    last = last * jnp.concatenate([edge[...], edge[...]], axis=0)
    last = dot(z_back[...], stacked(last))
    times_x(wide[:, :, :width])
    acc = jnp.zeros((depth, width), jnp.float32)
    for q in range(count):
        cos_part = wide[q, :, :width] + last[:, q : q + 1] * alternate
        sin_part = jnp.where(first, 0.0, wide[q, :, width:])
        real = cos_part[:depth] - sin_part[depth:]
        imag = cos_part[depth:] + sin_part[:depth]
        acc = acc + (held[q, :depth] * real + held[q, depth:] * imag)
        out[:, q, :] = real
        out[:, count + q, :] = imag
    energy[...] = jnp.full(energy.shape, jnp.sum(acc))


def filtered(spec, kernel_hat):
    depth, rows, width = spec.shape
    count = rows // 2
    edge = jnp.pad(kernel_hat[:, :, width], ((0, 0), (0, LANES - count)))
    tables = (*x_table(width), *z_tables(depth))
    whole = [pl.BlockSpec(array.shape, lambda i, r=array.ndim: (0,) * r) for array in tables]
    return pl.pallas_call(
        filter_kernel,
        grid=(1,),
        out_shape=(
            jax.ShapeDtypeStruct(spec.shape, jnp.float32),
            jax.ShapeDtypeStruct((SUBLANES, LANES), jnp.float32),
        ),
        in_specs=[
            pl.BlockSpec(spec.shape, lambda i: (0, 0, 0)),
            pl.BlockSpec((2 * depth, count, width), lambda i: (0, 0, 0)),
            pl.BlockSpec(edge.shape, lambda i: (0, 0)),
            *whole,
        ],
        out_specs=(
            pl.BlockSpec(spec.shape, lambda i: (0, 0, 0)),
            pl.BlockSpec((SUBLANES, LANES), lambda i: (0, 0)),
        ),
        scratch_shapes=[
            pltpu.VMEM((count, 2 * depth, width), jnp.float32),
            pltpu.VMEM((count, 2 * depth, 2 * width), jnp.float32),
        ],
        compiler_params=pltpu.CompilerParams(vmem_limit_bytes=VMEM_BYTES),
        cost_estimate=pl.CostEstimate(
            flops=10**10, bytes_accessed=4 * 10**6, transcendentals=0
        ),
        name="kernel_filter",
    )(spec, kernel_hat, edge, *tables)


def backward_kernel(
    devices, spec, v_rows, partial, t_high, t_low, v_out, h_out, e_out, gathered, sums, sends, receives
):
    me = lax.axis_index("gz")
    arrived = greet(devices)
    arrived()
    finish = remote(
        devices,
        [
            (lambda peer: spec.at[peer], lambda slot: gathered.at[slot]),
            (lambda peer: v_rows.at[:, peer], lambda slot: v_out.at[:, slot]),
            (lambda peer: partial, lambda slot: sums.at[slot]),
        ],
        sends,
        receives,
    )
    gathered[me] = spec[me]
    v_out[:, me] = v_rows[:, me]
    sums[me] = partial[...]
    finish()
    high, low = split(gathered[...].reshape(t_high.shape[1], spec.shape[2]))
    h_out[...] = dot(t_high[...], high) + (dot(t_high[...], low) + dot(t_low[...], high))
    e_out[...] = jnp.sum(sums[...], axis=0)


def backward_exchange(devices, spec, v_rows, partial, tables):
    width_y = tables[0].shape[0]
    return pl.pallas_call(
        functools.partial(backward_kernel, devices),
        out_shape=(
            jax.ShapeDtypeStruct(v_rows.shape, jnp.float32),
            jax.ShapeDtypeStruct((width_y, spec.shape[2]), jnp.float32),
            jax.ShapeDtypeStruct(partial.shape, jnp.float32),
        ),
        in_specs=[VMEM_SPEC] * 5,
        out_specs=(VMEM_SPEC,) * 3,
        scratch_shapes=[
            pltpu.VMEM(spec.shape, jnp.float32),
            pltpu.VMEM((devices, *partial.shape), jnp.float32),
            pltpu.SemaphoreType.DMA((3, devices)),
            pltpu.SemaphoreType.DMA((3, devices)),
        ],
        compiler_params=pltpu.CompilerParams(
            collective_id=1, has_side_effects=True, vmem_limit_bytes=VMEM_BYTES
        ),
        name="backward_exchange",
    )(spec, v_rows, partial, *tables)


def xc_rows(dens):
    stencil_reach = len(STENCIL)
    grad_z = plane_slope(dens, 1)
    grad_x = plane_slope(dens, 3)
    grad_y = inner_slope(extend_rows(dens, stencil_reach), 2)
    energy, d_dens, flux_z, flux_y, flux_x = xc_fields(dens, grad_z, grad_y, grad_x)
    divergence_y = inner_slope(extend_rows(flux_y, stencil_reach), 2)
    v_xc = d_dens - (plane_slope(flux_z, 1) + divergence_y + plane_slope(flux_x, 3))
    return v_xc, jnp.sum(energy)


def per_device(density, kernel_hat):
    planes, width_y, width_x = density.shape[1:]
    devices = lax.axis_size("gz")
    assert planes == 1
    depth_z = planes * devices
    cell_count = depth_z * width_y * width_x
    forward, inverse = y_tables(width_y, devices, 1.0 / (8 * cell_count))
    dens, spec = forward_exchange(
        devices, density.reshape(2, devices, width_y // devices, width_x), forward
    )
    v_rows, energy_xc = xc_rows(dens)
    back, energy_h = filtered(spec, kernel_hat)
    row = lax.broadcasted_iota(jnp.int32, energy_h.shape, 0)
    partial = jnp.where(
        row == 0, energy_xc / cell_count, energy_h * (0.5 / (8.0 * cell_count) / cell_count)
    )
    v_xc, hartree, sums = backward_exchange(devices, back, v_rows, partial, inverse)
    potential = v_xc.reshape(2, 1, width_y, width_x) + hartree[None, None]
    return (potential, sums[:2, 0])


def solution(mesh):
    placed = (P(None, "gz", None, None), P(None, "gz", None))
    return jax.shard_map(
        per_device,
        mesh=mesh,
        in_specs=placed,
        out_specs=(P(None, "gz", None, None), P()),
        check_vma=False,
    )
```

```python
import functools
import math

import jax
import jax.numpy as jnp
import numpy as np
from jax import lax
from jax.experimental import pallas as pl
from jax.experimental.pallas import tpu as pltpu
from jax.sharding import PartitionSpec as P

HGRID = 0.35
STENCIL = (0.8, -0.2, 4.0 / 105.0, -1.0 / 280.0)
KAPPA = 0.804
MU_X = 0.2195149727645171
BETA_C = 0.06672455060314922
GAMMA_C = 0.031090690869654894
FZ_CURV = 1.709921
PARAMS_UNPOL = (0.031091, 0.2137, 7.5957, 3.5876, 1.6382, 0.49294)
PARAMS_POL = (0.015545, 0.20548, 14.1189, 6.1977, 3.3662, 0.62517)
PARAMS_STIFF = (0.016887, 0.11125, 10.357, 3.6231, 0.88026, 0.49671)


def shifted(value, axis, steps):
    count = lax.axis_size(axis)
    leading, last = (max(0, -steps), min(count, count - steps))
    return lax.ppermute(value, axis, [(source, source + steps) for source in range(leading, last)])


def inner_slope(extended, direction):
    stencil_reach = len(STENCIL)
    length_out = extended.shape[direction] - 2 * stencil_reach
    result = 0.0
    for offset, weight in enumerate(STENCIL):
        upper_part = lax.slice_in_dim(
            extended,
            stencil_reach + offset + 1,
            stencil_reach + offset + 1 + length_out,
            axis=direction,
        )
        lower_part = lax.slice_in_dim(
            extended,
            stencil_reach - offset - 1,
            stencil_reach - offset - 1 + length_out,
            axis=direction,
        )
        result = result + weight * (upper_part - lower_part)
    return result / HGRID


def plane_slope(field, direction):
    stencil_reach = len(STENCIL)
    widths = [(0, 0)] * field.ndim
    widths[direction] = (stencil_reach, stencil_reach)
    return inner_slope(jnp.pad(field, widths), direction)


def pw_piece(radius, params):
    half_root = jnp.sqrt(radius)
    series = (
        params[2] * half_root
        + params[3] * radius
        + params[4] * radius * half_root
        + params[5] * radius * radius
    )
    return (
        -2.0 * params[0] * (1.0 + params[1] * radius) * jnp.log1p(1.0 / (2.0 * params[0] * series))
    )


def exchange_part(doubled, sigma_four):
    cube_root = jnp.cbrt(doubled)
    uniform_part = -0.75 * (3.0 / math.pi) ** (1.0 / 3.0) * cube_root
    reduced = sigma_four / (4.0 * (3.0 * math.pi**2) ** (2.0 / 3.0) * doubled**2 * cube_root**2)
    enhance = 1.0 + KAPPA - KAPPA / (1.0 + MU_X * reduced / KAPPA)
    return doubled * uniform_part * enhance


def energy_density(dens_up, dens_down, sigma_uu, sigma_ud, sigma_dd):
    exchange_term = 0.5 * exchange_part(2.0 * dens_up, 4.0 * sigma_uu) + 0.5 * exchange_part(
        2.0 * dens_down, 4.0 * sigma_dd
    )
    density_sum = dens_up + dens_down
    polarization = (dens_up - dens_down) / density_sum
    radius = jnp.cbrt(3.0 / (4.0 * math.pi * density_sum))
    plus_side = 1.0 + polarization
    minus_side = 1.0 - polarization
    plus_cube = jnp.cbrt(plus_side)
    minus_cube = jnp.cbrt(minus_side)
    spin_weight = (plus_side * plus_cube + minus_side * minus_cube - 2.0) / (
        2.0 ** (4.0 / 3.0) - 2.0
    )
    unpolar = pw_piece(radius, PARAMS_UNPOL)
    polarized = pw_piece(radius, PARAMS_POL)
    stiffness = pw_piece(radius, PARAMS_STIFF)
    polar_four = polarization**4
    local_corr = (
        unpolar
        - stiffness * spin_weight * (1.0 - polar_four) / FZ_CURV
        + (polarized - unpolar) * spin_weight * polar_four
    )
    phi_factor = 0.5 * (plus_cube**2 + minus_cube**2)
    phi_cubed = phi_factor**3
    screening_sq = 4.0 * jnp.cbrt(3.0 * math.pi**2 * density_sum) / math.pi
    sigma_total = sigma_uu + 2.0 * sigma_ud + sigma_dd
    scaled_sq = sigma_total / (4.0 * phi_factor**2 * screening_sq * density_sum**2)
    weight_a = BETA_C / GAMMA_C / jnp.expm1(-local_corr / (GAMMA_C * phi_cubed))
    gradient_term = (
        GAMMA_C
        * phi_cubed
        * jnp.log1p(
            BETA_C
            / GAMMA_C
            * scaled_sq
            * (1.0 + weight_a * scaled_sq)
            / (1.0 + weight_a * scaled_sq + weight_a**2 * scaled_sq**2)
        )
    )
    return exchange_term + density_sum * (local_corr + gradient_term)


def flux_pair(deriv_uu, deriv_ud, deriv_dd, gradient):
    return jnp.stack(
        [
            2.0 * deriv_uu * gradient[0] + deriv_ud * gradient[1],
            2.0 * deriv_dd * gradient[1] + deriv_ud * gradient[0],
        ]
    )


def xc_fields(dens, grad_z, grad_y, grad_x):
    sigma_uu = grad_z[0] * grad_z[0] + grad_y[0] * grad_y[0] + grad_x[0] * grad_x[0]
    sigma_ud = grad_z[0] * grad_z[1] + grad_y[0] * grad_y[1] + grad_x[0] * grad_x[1]
    sigma_dd = grad_z[1] * grad_z[1] + grad_y[1] * grad_y[1] + grad_x[1] * grad_x[1]
    energy, pullback = jax.vjp(energy_density, dens[0], dens[1], sigma_uu, sigma_ud, sigma_dd)
    d_up, d_down, d_uu, d_ud, d_dd = pullback(jnp.ones_like(energy))
    return (
        energy,
        jnp.stack([d_up, d_down]),
        flux_pair(d_uu, d_ud, d_dd, grad_z),
        flux_pair(d_uu, d_ud, d_dd, grad_y),
        flux_pair(d_uu, d_ud, d_dd, grad_x),
    )


MESH = pl.DeviceIdType.MESH
LANES = 128
SUBLANES = 8
VMEM_SPEC = pl.BlockSpec(memory_space=pltpu.VMEM)
VMEM_BYTES = 60 * 1024 * 1024


def extend_rows(field, depth):
    rows = field.shape[2]
    below_parts = []
    above_parts = []
    for distance in range(1, -(-depth // rows) + 1):
        needed = min(rows, depth - (distance - 1) * rows)
        below_parts.insert(0, shifted(field[:, :, rows - needed :], "gz", distance))
        above_parts.append(shifted(field[:, :, :needed], "gz", -distance))
    return jnp.concatenate(below_parts + [field] + above_parts, axis=2)


def split(value):
    high = value.astype(jnp.bfloat16)
    low = (value - high.astype(jnp.float32)).astype(jnp.bfloat16)
    return high, low


def np_split(table):
    table = np.asarray(table, np.float32)
    high = table.astype(jnp.bfloat16)
    low = (table - high.astype(np.float32)).astype(jnp.bfloat16)
    return high, low


def angles(spatial, spectral):
    index = np.outer(np.arange(spatial), np.arange(spectral)) % spectral
    return index * (2.0 * np.pi / spectral)


def y_tables(width_y, devices, scale):
    angle = angles(width_y, 2 * width_y)
    both = np.stack([np.cos(angle), -np.sin(angle)])
    both = both.reshape(2, width_y, devices, -1).transpose(2, 0, 3, 1)
    forward = both.reshape(4 * width_y, width_y)
    return np_split(forward), np_split(forward.T * scale)


def x_table(width_x):
    angle = angles(width_x, 2 * width_x)[:, :width_x]
    sine = np.sin(angle)
    sine[:, 0] = (-1.0) ** np.arange(width_x)
    return np_split(np.concatenate([np.cos(angle), sine], axis=1))


def z_tables(depth_z):
    angle = angles(depth_z, 2 * depth_z)
    cos, sin = np.cos(angle).T, np.sin(angle).T
    forward = np.block([[cos, sin], [-sin, cos]])
    out = []
    for table in (forward, forward.T):
        high, low = np_split(table)
        out.append(np.concatenate([high, high, low], axis=1))
    return out


def dot(left, right):
    return jnp.dot(left, right, preferred_element_type=jnp.float32)


def stacked(value):
    high, low = split(value)
    return jnp.concatenate([high, low, high], axis=0)


def greet(devices):
    me = lax.axis_index("gz")
    barrier = pltpu.get_barrier_semaphore()

    def signal(step, carry):
        pl.semaphore_signal(
            barrier,
            inc=1,
            device_id=(lax.rem(me + step, devices),),
            device_id_type=MESH,
        )
        return carry

    lax.fori_loop(1, devices, signal, 0)
    return lambda: pl.semaphore_wait(barrier, devices - 1)


def remote(devices, pieces, sends, receives):
    me = lax.axis_index("gz")

    def each(step, source_of, slot_of, act):
        for piece, (source, target) in enumerate(pieces):
            act(
                pltpu.make_async_remote_copy(
                    src_ref=source(source_of),
                    dst_ref=target(slot_of),
                    send_sem=sends.at[piece, step],
                    recv_sem=receives.at[piece, step],
                    device_id=(source_of,),
                    device_id_type=MESH,
                )
            )

    def start(step, carry):
        each(step, lax.rem(me + step, devices), me, lambda copy: copy.start())
        return carry

    def finish(step, carry):
        peer = lax.rem(me + step, devices)
        origin = lax.rem(me - step + devices, devices)
        each(step, peer, me, lambda copy: copy.wait_send())
        each(step, peer, origin, lambda copy: copy.wait_recv())
        return carry

    lax.fori_loop(1, devices, start, 0)
    return lambda: lax.fori_loop(1, devices, finish, 0)


def forward_kernel(devices, dens, t_high, t_low, dens_out, spec_out, spec, sends, receives):
    me = lax.axis_index("gz")
    arrived = greet(devices)
    width_y = t_high.shape[1]
    total = (dens[0] + dens[1]).reshape(width_y, dens.shape[3])
    high, low = split(total)
    values = dot(t_high[...], high) + (dot(t_high[...], low) + dot(t_low[...], high))
    spec[...] = values.reshape(spec.shape)
    arrived()
    finish = remote(
        devices,
        [
            (lambda peer: dens.at[:, peer], lambda slot: dens_out.at[:, slot]),
            (lambda peer: spec.at[peer], lambda slot: spec_out.at[slot]),
        ],
        sends,
        receives,
    )
    dens_out[:, me] = dens[:, me]
    spec_out[me] = spec[me]
    finish()


def forward_exchange(devices, dens, tables):
    width_x = dens.shape[3]
    spec_shape = (devices, tables[0].shape[0] // devices, width_x)
    return pl.pallas_call(
        functools.partial(forward_kernel, devices),
        out_shape=(
            jax.ShapeDtypeStruct(dens.shape, jnp.float32),
            jax.ShapeDtypeStruct(spec_shape, jnp.float32),
        ),
        in_specs=[VMEM_SPEC] * 3,
        out_specs=(VMEM_SPEC, VMEM_SPEC),
        scratch_shapes=[
            pltpu.VMEM(spec_shape, jnp.float32),
            pltpu.SemaphoreType.DMA((2, devices)),
            pltpu.SemaphoreType.DMA((2, devices)),
        ],
        compiler_params=pltpu.CompilerParams(
            collective_id=0, has_side_effects=True, vmem_limit_bytes=VMEM_BYTES
        ),
        name="forward_exchange",
    )(dens, *tables)


def filter_kernel(spec, kernel_hat, edge, tx_high, tx_low, z_fore, z_back, out, energy, held, wide):
    depth, rows, width = spec.shape
    count = rows // 2
    for q in range(count):
        held[q, :depth] = spec[:, q, :]
        held[q, depth:] = spec[:, count + q, :]

    def times_x(value):
        high, low = split(value.reshape(count * 2 * depth, width))
        result = dot(high, tx_high[...]) + (dot(low, tx_high[...]) + dot(high, tx_low[...]))
        wide[...] = result.reshape(wide.shape)

    lane = lax.broadcasted_iota(jnp.int32, (1, width), 1)
    first = lane == 0
    weight = jnp.where(first, 1.0, 2.0)
    alternate = jnp.where(lane % 2 == 0, 1.0, -1.0)
    edge_lane = lax.broadcasted_iota(jnp.int32, (1, LANES), 1)
    times_x(held[...])
    last = jnp.zeros((2 * depth, LANES), jnp.float32)
    back = []
    for q in range(count):
        cos_part = wide[q, :, :width]
        sin_part = wide[q, :, width:]
        last = jnp.where(edge_lane == q, sin_part[:, :1], last)
        sin_part = jnp.where(first, 0.0, sin_part)
        value = jnp.concatenate(
            [cos_part[:depth] + sin_part[depth:], cos_part[depth:] - sin_part[:depth]], axis=0
        )
        value = dot(z_fore[...], stacked(value))
        factor = kernel_hat[:, q, :] * weight
        value = value * jnp.concatenate([factor, factor], axis=0)
        wide[q, :, :width] = dot(z_back[...], stacked(value))
    last = dot(z_fore[...], stacked(last))
    last = last * jnp.concatenate([edge[...], edge[...]], axis=0)
    last = dot(z_back[...], stacked(last))
    times_x(wide[:, :, :width])
    acc = jnp.zeros((depth, width), jnp.float32)
    for q in range(count):
        cos_part = wide[q, :, :width] + last[:, q : q + 1] * alternate
        sin_part = jnp.where(first, 0.0, wide[q, :, width:])
        real = cos_part[:depth] - sin_part[depth:]
        imag = cos_part[depth:] + sin_part[:depth]
        acc = acc + (held[q, :depth] * real + held[q, depth:] * imag)
        out[:, q, :] = real
        out[:, count + q, :] = imag
    energy[...] = jnp.full(energy.shape, jnp.sum(acc))


def filtered(spec, kernel_hat):
    depth, rows, width = spec.shape
    count = rows // 2
    edge = jnp.pad(kernel_hat[:, :, width], ((0, 0), (0, LANES - count)))
    tables = (*x_table(width), *z_tables(depth))
    whole = [pl.BlockSpec(array.shape, lambda i, r=array.ndim: (0,) * r) for array in tables]
    return pl.pallas_call(
        filter_kernel,
        grid=(1,),
        out_shape=(
            jax.ShapeDtypeStruct(spec.shape, jnp.float32),
            jax.ShapeDtypeStruct((SUBLANES, LANES), jnp.float32),
        ),
        in_specs=[
            pl.BlockSpec(spec.shape, lambda i: (0, 0, 0)),
            pl.BlockSpec((2 * depth, count, width), lambda i: (0, 0, 0)),
            pl.BlockSpec(edge.shape, lambda i: (0, 0)),
            *whole,
        ],
        out_specs=(
            pl.BlockSpec(spec.shape, lambda i: (0, 0, 0)),
            pl.BlockSpec((SUBLANES, LANES), lambda i: (0, 0)),
        ),
        scratch_shapes=[
            pltpu.VMEM((count, 2 * depth, width), jnp.float32),
            pltpu.VMEM((count, 2 * depth, 2 * width), jnp.float32),
        ],
        compiler_params=pltpu.CompilerParams(vmem_limit_bytes=VMEM_BYTES),
        cost_estimate=pl.CostEstimate(
            flops=10**10, bytes_accessed=4 * 10**6, transcendentals=0
        ),
        name="kernel_filter",
    )(spec, kernel_hat, edge, *tables)


def backward_kernel(
    devices, spec, v_rows, partial, t_high, t_low, out, e_out, v_all, sums, sends, receives
):
    me = lax.axis_index("gz")
    greet(devices)()
    finish = remote(
        devices,
        [
            (lambda peer: v_rows.at[:, peer], lambda slot: v_all.at[:, slot]),
            (lambda peer: partial, lambda slot: sums.at[slot]),
        ],
        sends,
        receives,
    )
    v_all[:, me] = v_rows[:, me]
    sums[me] = partial[...]
    high, low = split(spec[...].reshape(t_high.shape[1], spec.shape[2]))
    values = dot(t_high[...], high) + (dot(t_high[...], low) + dot(t_low[...], high))
    out[0] = values.reshape(out.shape[1:])
    finish()
    e_out[...] = jnp.sum(sums[...], axis=0)
    values = out[0]
    out[0] = values + v_all[0]
    out[1] = values + v_all[1]


def backward_exchange(devices, spec, v_rows, partial, tables):
    return pl.pallas_call(
        functools.partial(backward_kernel, devices),
        out_shape=(
            jax.ShapeDtypeStruct(v_rows.shape, jnp.float32),
            jax.ShapeDtypeStruct(partial.shape, jnp.float32),
        ),
        in_specs=[VMEM_SPEC] * 5,
        out_specs=(VMEM_SPEC,) * 2,
        scratch_shapes=[
            pltpu.VMEM(v_rows.shape, jnp.float32),
            pltpu.VMEM((devices, *partial.shape), jnp.float32),
            pltpu.SemaphoreType.DMA((2, devices)),
            pltpu.SemaphoreType.DMA((2, devices)),
        ],
        compiler_params=pltpu.CompilerParams(
            collective_id=1, has_side_effects=True, vmem_limit_bytes=VMEM_BYTES
        ),
        name="backward_exchange",
    )(spec, v_rows, partial, *tables)


def xc_rows(dens, extended):
    stencil_reach = len(STENCIL)
    grad_z = plane_slope(dens, 1)
    grad_x = plane_slope(dens, 3)
    grad_y = inner_slope(extended, 2)
    energy, d_dens, flux_z, flux_y, flux_x = xc_fields(dens, grad_z, grad_y, grad_x)
    divergence_y = inner_slope(extend_rows(flux_y, stencil_reach), 2)
    v_xc = d_dens - (plane_slope(flux_z, 1) + divergence_y + plane_slope(flux_x, 3))
    return v_xc, jnp.sum(energy)


def per_device(density, kernel_hat):
    planes, width_y, width_x = density.shape[1:]
    devices = lax.axis_size("gz")
    assert planes == 1
    depth_z = planes * devices
    cell_count = depth_z * width_y * width_x
    forward, inverse = y_tables(width_y, devices, 1.0 / (8 * cell_count))
    dens, spec = forward_exchange(
        devices, density.reshape(2, devices, width_y // devices, width_x), forward
    )
    extended = extend_rows(dens, len(STENCIL))
    back, energy_h = filtered(spec, kernel_hat)
    dens, extended, back = lax.optimization_barrier((dens, extended, back))
    back = lax.all_to_all(back, "gz", split_axis=0, concat_axis=0, tiled=True)
    v_rows, energy_xc = xc_rows(dens, extended)
    row = lax.broadcasted_iota(jnp.int32, energy_h.shape, 0)
    partial = jnp.where(
        row == 0, energy_xc / cell_count, energy_h * (0.5 / (8.0 * cell_count) / cell_count)
    )
    potential, sums = backward_exchange(devices, back, v_rows, partial, inverse)
    return (potential.reshape(density.shape), sums[:2, 0])


def solution(mesh):
    placed = (P(None, "gz", None, None), P(None, "gz", None))
    return jax.shard_map(
        per_device,
        mesh=mesh,
        in_specs=placed,
        out_specs=(P(None, "gz", None, None), P()),
        check_vma=False,
    )
```
